256 devices in a mesh: group: 2 (over y), tensor: 32 (over z, core), seq: 4 (over x).
Axes of the slice: x: 4, y: 2, z: 16, core: 2. Of those that a mesh axis runs over, the one named last changes fastest.
The devices are a block of a 4x16x16 slice.
Arguments:
- mixer_input: bfloat16 [2048, 8192], P(('group', 'seq'), 'tensor'), parts along dimension 0, may hold values from -6 to 6
- state_maps: bfloat16 [2048, 256], P(('group', 'seq')), parts along dimension 0, may hold values from -6 to 6
- gate_input: bfloat16 [2048, 8192], P(('group', 'seq'), 'tensor'), parts along dimension 0, may hold values from -6 to 6
- step_raw: float32 [128, 2048], P('tensor', ('group', 'seq')), parts along dimension 1, may hold values from -10 to 10, as said below
- decay_log: float32 [128], P('tensor'), may hold values from -4 to -2
- skip_gain: float32 [128], P('tensor'), may hold values from 0.5 to 1.5
- conv_input: bfloat16 [4, 8192], P(None, 'tensor'), may hold values from -3 to 3
- conv_maps: bfloat16 [4, 256], replicated, may hold values from -3 to 3
- norm_gain: float32 [8192], P('tensor'), may hold values from 0.1 to 1.9
- out_weight: bfloat16 [8192, 8192], P('tensor'), may hold values from -0.125 to 0.125
Outputs:
- mixed: bfloat16 [2048, 8192], P(('group', 'seq'), 'tensor'), parts along dimension 0
The draws below stay inside these ranges and needn't reach their ends.
There are 2 independent parts, one for each index of `group`. The reference program is written for one: setup_inputs(seed, part) draws one part's arguments, and reference() takes and returns one part's arrays. A program takes and returns all parts, laid end to end along the dimension named above; an argument that names none is the same for every part. Nothing has to cross between parts.
Inputs may be any that keep to these rules, and one draw needn't show every extreme that they name: `step_raw`: Real-valued step parameters before softplus.
All inputs are finite; a program needn't handle non-finite values.
Results may differ from the reference program's by a relative error of at most 0.008.
Values may be sent and summed in bfloat16 or wider, within the bound.
No kernel may reach another device: no remote copies, remote signals or barrier semaphores. Data moves between devices by JAX's collectives and lax.ppermute only.
A program may use at most 64 MiB of HBM per device.

```python
import jax
import jax.numpy as jnp
from jax import lax

D = 8192
HEAD_TOTAL = 128
HEAD_DIM = 64
STATE = 128
CONV = 4
SPAN = 256
TOKENS_PER_SHARD = 256
INNER = 8192
SEQUENCE_LENGTH = 1024


def draw_step_raw(key, part):
    tensor_dims = (HEAD_TOTAL, SEQUENCE_LENGTH)
    kind_key = jax.random.fold_in(key, 31)
    slow_key = jax.random.fold_in(key, 32)
    fast_key = jax.random.fold_in(key, 33)
    spike_frequency_key = jax.random.fold_in(key, 34)
    spike_location_key = jax.random.fold_in(key, 35)
    spike_magnitude_key = jax.random.fold_in(key, 36)
    share_fast = 0.5
    fast_heads = jax.random.uniform(kind_key, (HEAD_TOTAL, 1), jnp.float32) < share_fast
    gradual_baseline = jax.random.uniform(slow_key, tensor_dims, jnp.float32, -9.0, -7.0)
    fast_base = jax.random.uniform(fast_key, tensor_dims, jnp.float32, 0.0, 3.0)
    segment_pieces = SEQUENCE_LENGTH // TOKENS_PER_SHARD
    segment_frequency = jax.random.uniform(spike_frequency_key, (HEAD_TOTAL, segment_pieces, 1), jnp.float32, 0.0, 3.0) / TOKENS_PER_SHARD
    position_frequency = jnp.broadcast_to(segment_frequency, (HEAD_TOTAL, segment_pieces, TOKENS_PER_SHARD)).reshape(tensor_dims)
    spike_events = jax.random.uniform(spike_location_key, tensor_dims, jnp.float32) < position_frequency
    spike_amounts = jax.random.uniform(spike_magnitude_key, tensor_dims, jnp.float32, 4.0, 6.0)
    gradual_amounts = jnp.where(spike_events, spike_amounts, gradual_baseline)
    return jnp.where(fast_heads, fast_base, gradual_amounts).astype(jnp.float32)


def spiked(array, key, source, target, parts, factor):
    owner, partner = [(jnp.arange(array.shape[dim]) // (array.shape[dim] // parts)).reshape([-1 if axis == dim else 1 for axis in range(array.ndim)]) for dim in (source, target)]
    chosen = jax.random.permutation(key, parts)[partner]
    strong = (owner == chosen) | (owner == (partner + parts // 2) % parts)
    return jnp.where(strong, factor * array, array)


def steps_of(own_key, shape, pieces, least, largest):
    def one(position, blocks):
        heights = jax.random.uniform(jax.random.fold_in(jax.random.fold_in(own_key, 6), position), (blocks,), jnp.float32, least / len(pieces), largest / len(pieces))
        return jnp.repeat(jnp.exp(heights), shape[position] // blocks).reshape((-1,) + (1,) * (len(shape) - position - 1))

    factor_of = one(*pieces[0])
    for cut in pieces[1:]:
        factor_of = factor_of * one(*cut)
    return factor_of


def centred(own_key, extent, width, most, shards=(), held_as=jnp.bfloat16):
    entries = jax.random.normal(own_key, extent, jnp.float32) * width
    if len(shards) > 0:
        entries = steps_of(own_key, extent, shards, -0.22, 0.18) * entries
    return jnp.clip(entries, min=-most, max=most).astype(held_as)


def bell_draw_with(rng, extent, deviation, bound, shards, heavy, kind=jnp.bfloat16):
    result = deviation * jax.random.normal(rng, extent, jnp.float32)
    if shards:
        result = result * steps_of(rng, extent, shards, -0.22, 0.18)
    return jnp.clip(spiked(result, jax.random.fold_in(rng, 3), *heavy), -bound, bound).astype(kind)


def setup_inputs(seed: int = 0, part: int = 0) -> dict:
    keys = jax.random.split(jax.random.key(seed), 11)
    part_splits = jax.random.split(jax.random.fold_in(keys[10], part), 11)
    mixer_input = centred(part_splits[0], (SEQUENCE_LENGTH, INNER), 1.0, 6.0, ((0, 4), (1, 32)))
    state_maps = centred(part_splits[1], (SEQUENCE_LENGTH, 2 * STATE), 1.0, 6.0, ((0, 4),))
    gate_input = centred(part_splits[2], (SEQUENCE_LENGTH, INNER), 1.0, 6.0, ((0, 4), (1, 32)))
    step_raw = draw_step_raw(jax.random.fold_in(jax.random.fold_in(keys[10], part), 71), part)
    decay_log = jnp.clip(-4.0 + 2.0 * jax.random.uniform(keys[4], (HEAD_TOTAL,), jnp.float32) ** steps_of(keys[4], (HEAD_TOTAL,), ((0, 32),), -0.2, 0.2), -4.0, -2.0)
    skip_gain = jnp.clip(0.5 + 1.0 * jax.random.uniform(keys[5], (HEAD_TOTAL,), jnp.float32) ** steps_of(keys[5], (HEAD_TOTAL,), ((0, 32),), -0.2, 0.2), 0.5, 1.5)
    conv_input = centred(keys[6], (CONV, INNER), CONV ** -0.5, 3.0, ((1, 32),))
    conv_maps = centred(keys[7], (CONV, 2 * STATE), CONV ** -0.5, 3.0)
    norm_gain = jnp.clip(1.0 + 0.18 * jax.random.normal(keys[8], (INNER,), jnp.float32), 0.1, 1.9)
    out_weight = bell_draw_with(keys[9], (INNER, D), INNER ** -0.5, 0.125, ((0, 32),), (0, 1, 32, 2.75))
    return dict(mixer_input=mixer_input, state_maps=state_maps, gate_input=gate_input, step_raw=step_raw, decay_log=decay_log, skip_gain=skip_gain, conv_input=conv_input, conv_maps=conv_maps, norm_gain=norm_gain, out_weight=out_weight)


PRECISE = lax.Precision.HIGHEST

def causal_conv(values, kernel):
    widened = values.astype(jnp.float32)
    padded = jnp.concatenate([jnp.zeros((CONV - 1, widened.shape[1]), jnp.float32), widened], axis=0)
    summed = jnp.zeros(widened.shape, jnp.float32)
    for offset in range(CONV):
        summed = summed + kernel[offset].astype(jnp.float32) * padded[offset:offset + widened.shape[0]]
    return jax.nn.silu(summed).astype(jnp.bfloat16)

def reference(mixer_input, state_maps, gate_input, step_raw, decay_log, skip_gain, conv_input, conv_maps, norm_gain, out_weight):
    conv_out = causal_conv(mixer_input, conv_input)
    maps_out = causal_conv(state_maps, conv_maps)
    blocks = SEQUENCE_LENGTH // SPAN
    b_blocks = maps_out[:, :STATE].astype(jnp.float32).reshape(blocks, SPAN, STATE)
    c_blocks = maps_out[:, STATE:].astype(jnp.float32).reshape(blocks, SPAN, STATE)
    scores = jnp.einsum('ktn,ksn->kts', c_blocks, b_blocks, precision=PRECISE)
    step_size = jax.nn.softplus(step_raw)
    rates = jnp.exp(decay_log)
    causal = jnp.arange(SPAN)[:, None] >= jnp.arange(SPAN)[None, :]
    heads_first = conv_out.reshape(SEQUENCE_LENGTH, HEAD_TOTAL, HEAD_DIM).transpose(1, 0, 2)

    def one_head(operands):
        values, step_sizes, decay_rate, skip_scale = operands
        log_decay = -decay_rate * step_sizes
        cumulative = jnp.cumsum(log_decay.reshape(blocks, SPAN), axis=1)
        step_blocks = step_sizes.reshape(blocks, SPAN)
        value_blocks = values.astype(jnp.float32).reshape(blocks, SPAN, HEAD_DIM)
        logarithm_spacing = jnp.where(causal, cumulative[:, :, None] - cumulative[:, None, :], 0.0)
        weights = jnp.where(causal, scores * jnp.exp(logarithm_spacing) * step_blocks[:, None, :], 0.0).astype(jnp.bfloat16)
        inside = jnp.einsum('kts,ksp->ktp', weights.astype(jnp.float32), value_blocks, precision=PRECISE)
        tail_weight = jnp.exp(cumulative[:, -1:] - cumulative) * step_blocks
        block_states = jnp.einsum('ksp,ksn->kpn', value_blocks * tail_weight[:, :, None], b_blocks, precision=PRECISE)

        def advance(state_now, element):
            decay_now, block_add = element
            return (decay_now * state_now + block_add, state_now)
        _, carried = lax.scan(advance, jnp.zeros((HEAD_DIM, STATE), jnp.float32), (jnp.exp(cumulative[:, -1]), block_states))
        carried_part = jnp.einsum('ktn,kpn->ktp', c_blocks, carried, precision=PRECISE) * jnp.exp(cumulative)[:, :, None]
        return (inside + carried_part + skip_scale * value_blocks).reshape(SEQUENCE_LENGTH, HEAD_DIM)
    scanned = lax.map(one_head, (heads_first, step_size, rates, skip_gain))
    scanned = scanned.transpose(1, 0, 2).reshape(SEQUENCE_LENGTH, INNER)
    gated_values = scanned * jax.nn.silu(gate_input.astype(jnp.float32))
    grouped = gated_values.reshape(SEQUENCE_LENGTH, HEAD_TOTAL, HEAD_DIM)
    inverse_root_mean = lax.rsqrt(lax.optimization_barrier(jnp.mean(grouped * grouped, axis=2, keepdims=True)) + 1e-05)
    normed = ((grouped * inverse_root_mean).reshape(SEQUENCE_LENGTH, INNER) * norm_gain).astype(jnp.bfloat16)
    return jnp.dot(normed, out_weight, preferred_element_type=jnp.float32).astype(jnp.bfloat16)
```

```python
import functools

import jax
import jax.numpy as jnp
from jax import lax
from jax.experimental import pallas as pl
from jax.experimental.pallas import tpu as pltpu
from jax.sharding import PartitionSpec as P

SPAN = 256
CORES = 2


PRECISE = lax.Precision.HIGHEST


def shifted(shard, axis, by):
    devices = lax.axis_size(axis)
    pairs = [(i, i + by) for i in range(devices) if 0 <= i + by < devices]
    return lax.ppermute(shard, axis, pairs)


def to_other_core(shard):
    devices = lax.axis_size("tensor")
    return lax.ppermute(shard, "tensor", [(i, i ^ 1) for i in range(devices)])


def to_chip(shard, by):
    devices = lax.axis_size("tensor")
    return lax.ppermute(
        shard, "tensor", [(i, (i + CORES * by) % devices) for i in range(devices)]
    )


def causal_conv(leading, values, kernel):
    padded = jnp.concatenate([leading, values], axis=0).astype(jnp.float32)
    summed = jnp.zeros(values.shape, jnp.float32)
    for offset in range(kernel.shape[0]):
        summed = (
            summed + kernel[offset].astype(jnp.float32) * padded[offset : offset + values.shape[0]]
        )
    return jax.nn.silu(summed).astype(jnp.bfloat16)


def product_kernel(blocks, own_values, other_values, own_weight, other_weight, out):
    out[0] = jnp.dot(
        own_values[...], own_weight[...], preferred_element_type=jnp.float32
    ) + jnp.dot(other_values[...], other_weight[...], preferred_element_type=jnp.float32)


def products(blocks, own_values, other_values, own_weight, other_weight, width):
    count = blocks.shape[0]
    rows, depth = own_values.shape
    whole = pl.BlockSpec((rows, depth), lambda i, at: (0, 0))
    column = pl.BlockSpec((depth, width), lambda i, at: (0, at[i]))
    return pl.pallas_call(
        product_kernel,
        grid_spec=pltpu.PrefetchScalarGridSpec(
            num_scalar_prefetch=1,
            grid=(count,),
            in_specs=[whole, whole, column, column],
            out_specs=pl.BlockSpec((1, rows, width), lambda i, at: (i, 0, 0)),
        ),
        out_shape=jax.ShapeDtypeStruct((count, rows, width), jnp.float32),
        compiler_params=pltpu.CompilerParams(vmem_limit_bytes=8 << 20),
        cost_estimate=pl.CostEstimate(
            flops=count * 4 * rows * depth * width,
            bytes_accessed=count * (4 * depth * width + 4 * rows * width),
            transcendentals=0,
        ),
    )(blocks, own_values, other_values, own_weight, other_weight)


def project(normed, out_weight, other_weight):
    devices = lax.axis_size("tensor")
    chips = devices // CORES
    me = lax.axis_index("tensor")
    width = out_weight.shape[1] // devices
    other = to_other_core(normed)
    far = chips // 2

    def block_of(by):
        return lax.rem(me + CORES * (by + chips), devices)

    order = [far, 1 - far]
    for step in range(1, far):
        order.append(far - step)
        if step + 1 < far:
            order.append(step + 1 - far)
    order.append(0)
    first = products(
        jnp.stack([block_of(by) for by in order[:2]]),
        normed, other, out_weight, other_weight, width,
    )
    rest = products(
        jnp.stack([block_of(by) for by in order[2:]]),
        normed, other, out_weight, other_weight, width,
    )
    part = {by: (first[i] if i < 2 else rest[i - 2]) for i, by in enumerate(order)}
    up = part[far].astype(jnp.bfloat16)
    down = part[1 - far].astype(jnp.bfloat16)
    for step in range(1, far):
        up = to_chip(up, 1)
        down = to_chip(down, -1)
        up = (up.astype(jnp.float32) + part[far - step]).astype(jnp.bfloat16)
        if step + 1 < far:
            down, up = lax.optimization_barrier((down, up))
            down = (down.astype(jnp.float32) + part[step + 1 - far]).astype(jnp.bfloat16)
    up = to_chip(up, 1)
    total = part[0] + down.astype(jnp.float32)
    return (total + up.astype(jnp.float32)).astype(jnp.bfloat16)


def local(
    mixer_input,
    state_maps,
    gate_input,
    step_raw,
    decay_log,
    skip_gain,
    conv_input,
    conv_maps,
    norm_gain,
    out_weight,
):
    tokens, channels = mixer_input.shape
    resident_heads = decay_log.shape[0]
    head_dim = channels // resident_heads
    state_dim = state_maps.shape[1] // 2
    lead_rows = conv_input.shape[0] - 1
    tail_rows = jnp.concatenate(
        [mixer_input[tokens - lead_rows :], state_maps[tokens - lead_rows :]], axis=1
    )
    leading = shifted(tail_rows, "seq", 1)
    other_weight = to_other_core(out_weight)
    conv_out = causal_conv(leading[:, :channels], mixer_input, conv_input)
    maps_out = causal_conv(leading[:, channels:], state_maps, conv_maps)
    b_maps = maps_out[:, :state_dim]
    c_maps = maps_out[:, state_dim:]
    scores = jnp.einsum("tn,sn->ts", c_maps, b_maps, preferred_element_type=jnp.float32)
    step_size = jax.nn.softplus(step_raw)
    log_decay = -jnp.exp(decay_log)[:, None] * step_size
    cumulative = jnp.cumsum(log_decay, axis=1)
    causal = lax.broadcasted_iota(jnp.int32, (SPAN, SPAN), 0) >= lax.broadcasted_iota(
        jnp.int32, (SPAN, SPAN), 1
    )
    logarithm_spacing = jnp.where(causal, cumulative[:, :, None] - cumulative[:, None, :], 0.0)
    weights = jnp.where(
        causal, scores[None] * jnp.exp(logarithm_spacing) * step_size[:, None, :], 0.0
    ).astype(jnp.bfloat16)
    values = conv_out.reshape(tokens, resident_heads, head_dim)
    inside = jnp.einsum("hts,shp->thp", weights, values, preferred_element_type=jnp.float32)
    tail_weight = jnp.exp(cumulative[:, -1:] - cumulative) * step_size
    weighted = values.astype(jnp.float32) * tail_weight.T[:, :, None]
    end_state = jnp.einsum("shp,sn->hpn", weighted, b_maps.astype(jnp.float32), precision=PRECISE)
    device_decay = jnp.exp(cumulative[:, -1])
    sent = jnp.concatenate(
        [end_state.reshape(channels, state_dim),
         jnp.broadcast_to(device_decay[:, None], (resident_heads, state_dim))], axis=0
    )
    behind = [shifted(sent, "seq", by) for by in range(1, lax.axis_size("seq"))]
    carried = jnp.zeros((resident_heads, head_dim, state_dim), jnp.float32)
    for message in behind[::-1]:
        state = message[:channels].reshape(resident_heads, head_dim, state_dim)
        carried = message[channels:, :1, None] * carried + state
    growth = jnp.exp(cumulative).T[:, :, None]
    carried_part = (
        jnp.einsum("tn,hpn->thp", c_maps.astype(jnp.float32), carried, precision=PRECISE) * growth
    )
    scanned = inside + carried_part + skip_gain[None, :, None] * values.astype(jnp.float32)
    gate_values = jax.nn.silu(gate_input.astype(jnp.float32)).reshape(
        tokens, resident_heads, head_dim
    )
    gated_values = scanned * gate_values
    inverse_root_mean = lax.rsqrt(
        jnp.mean(gated_values * gated_values, axis=2, keepdims=True) + 1e-05
    )
    normed = ((gated_values * inverse_root_mean).reshape(tokens, channels) * norm_gain).astype(
        jnp.bfloat16
    )
    return project(normed, out_weight, other_weight)


def solution(mesh):
    placed = (
        P(("group", "seq"), "tensor"),
        P(("group", "seq"), None),
        P(("group", "seq"), "tensor"),
        P("tensor", ("group", "seq")),
        P("tensor"),
        P("tensor"),
        P(None, "tensor"),
        P(),
        P("tensor"),
        P("tensor", None),
    )
    return jax.shard_map(
        local, mesh=mesh, in_specs=placed, out_specs=P(("group", "seq"), "tensor"), check_vma=False
    )
```

```python
import functools

import jax
import jax.numpy as jnp
from jax import lax
from jax.experimental import pallas as pl
from jax.experimental.pallas import tpu as pltpu
from jax.sharding import PartitionSpec as P


CORES = 2
STREAMS = 2
LEAD = 16
F32 = jnp.float32
BF16 = jnp.bfloat16
PRECISE = lax.Precision.HIGHEST
VMEM = pl.BlockSpec(memory_space=pltpu.VMEM)
SMEM = pl.BlockSpec(memory_space=pltpu.SMEM)
HBM = pl.BlockSpec(memory_space=pltpu.HBM)


def shifted(shard, axis, by):
    devices = lax.axis_size(axis)
    pairs = [(i, i + by) for i in range(devices) if 0 <= i + by < devices]
    return lax.ppermute(shard, axis, pairs)


def to_other_core(shard):
    devices = lax.axis_size("tensor")
    return lax.ppermute(shard, "tensor", [(i, i ^ 1) for i in range(devices)])


def to_chip(shard, by):
    devices = lax.axis_size("tensor")
    return lax.ppermute(
        shard, "tensor", [(i, (i + CORES * by) % devices) for i in range(devices)]
    )


def call(body, specs, shapes, flops, scratch=()):
    return pl.pallas_call(
        body,
        in_specs=specs,
        out_specs=tuple(VMEM for _ in shapes),
        out_shape=tuple(jax.ShapeDtypeStruct(s, d) for s, d in shapes),
        scratch_shapes=list(scratch),
        compiler_params=pltpu.CompilerParams(vmem_limit_bytes=16 << 20),
        cost_estimate=pl.CostEstimate(flops=flops, bytes_accessed=1 << 20, transcendentals=0),
    )


def along(a, b, ca, cb, precision=None):
    return lax.dot_general(
        a, b, (((ca,), (cb,)), ((), ())), preferred_element_type=F32, precision=precision
    )


def halves(x):
    high = x.astype(BF16)
    return high, (x - high.astype(F32)).astype(BF16)


def silu(v):
    return v / (1.0 + jnp.exp(-v))


def per_head(columns, rows, width, head_dim):
    lane = lax.broadcasted_iota(jnp.int32, (rows, width), 1) // head_dim
    spread = jnp.broadcast_to(columns[:, 0:1], (rows, width))
    for head in range(1, width // head_dim):
        spread = jnp.where(lane == head, columns[:, head : head + 1], spread)
    return spread


def tail_body(mixer, maps, out, sems):
    tokens, width = mixer.shape
    rows = pl.ds(tokens - LEAD, LEAD)
    copies = [
        pltpu.make_async_copy(mixer.at[rows], out.at[:, pl.ds(0, width)], sems.at[0]),
        pltpu.make_async_copy(maps.at[rows], out.at[:, pl.ds(width, maps.shape[1])], sems.at[1]),
    ]
    for copy in copies:
        copy.start()
    for copy in copies:
        copy.wait()


def tail_of(mixer_input, state_maps):
    width = mixer_input.shape[1] + state_maps.shape[1]
    return call(
        tail_body, [HBM, HBM], [((LEAD, width), BF16)], 1000, [pltpu.SemaphoreType.DMA((2,))]
    )(mixer_input, state_maps)[0]


def decay_body(
    heads, head_dim, step_hbm, decay_hbm, skip_hbm, gate_hbm, mixer_hbm, maps_hbm, taps_hbm,
    map_taps_hbm, mix, tail, growth, ends, gated, skip, summed,
    raw, logs, gains, gate, mixer, maps, taps, map_taps, padded, sems
):
    pairs = [(decay_hbm, logs), (step_hbm, raw), (skip_hbm, gains), (gate_hbm, gate),
             (taps_hbm, taps), (map_taps_hbm, map_taps), (mixer_hbm, mixer), (maps_hbm, maps)]
    copies = [pltpu.make_async_copy(a, b, sems.at[i]) for i, (a, b) in enumerate(pairs)]
    for copy in copies:
        copy.start()
    tokens = raw.shape[1]
    width = heads * head_dim
    row = lax.broadcasted_iota(jnp.int32, (heads, tokens), 0)
    to = lax.broadcasted_iota(jnp.int32, (tokens, tokens), 0)
    since = lax.broadcasted_iota(jnp.int32, (tokens, tokens), 1)
    causal = to >= since
    ones = jnp.where(causal, 1.0, 0.0).astype(F32)
    same = jnp.where(to == since, 1.0, 0.0).astype(F32)
    for copy in copies[:3]:
        copy.wait()
    step = jnp.maximum(raw[...], 0.0) + jnp.log1p(jnp.exp(-jnp.abs(raw[...])))
    rates = jnp.broadcast_to(logs[:, 0:1], (heads, tokens))
    for head in range(1, heads):
        rates = jnp.where(row == head, logs[:, head : head + 1], rates)
    change = -jnp.exp(rates) * step
    across = along(change, ones, 1, 1, PRECISE)
    down = along(ones, change, 1, 1, PRECISE)
    step_down = along(same, step, 1, 1, PRECISE)
    for head in range(heads):
        spacing = jnp.where(causal, down[:, head : head + 1] - across[head : head + 1, :], -1e30)
        mix[head] = jnp.exp(spacing) * step[head : head + 1, :]
    last = down[tokens - 1 : tokens, :]
    tail[...] = per_head(jnp.exp(last - down) * step_down, tokens, width, head_dim)
    growth[...] = per_head(jnp.exp(down), tokens, width, head_dim)
    ends[...] = jnp.broadcast_to(jnp.exp(across[:, tokens - 1 : tokens]), ends.shape)
    skip[...] = per_head(gains[...], 1, width, head_dim)
    for copy in copies[3:]:
        copy.wait()
    gated[...] = silu(gate[...].astype(F32))
    for source, kernel, first in ((mixer, taps, 0), (maps, map_taps, width)):
        count = kernel.shape[0]
        columns = source.shape[1]
        padded[0:8, :columns] = jnp.zeros((8, columns), F32)
        padded[8 : 8 + tokens, :columns] = source[...].astype(F32)
        total = None
        for tap in range(count):
            at = 9 - count + tap
            term = kernel[tap : tap + 1, :].astype(F32) * padded[at : at + tokens, :columns]
            total = term if total is None else total + term
        summed[:, first : first + columns] = total


def decay(step_raw, decay_log, skip_gain, gate_input, mixer_input, state_maps, conv_input,
          conv_maps):
    heads, tokens = step_raw.shape
    channels = mixer_input.shape[1]
    square = (tokens, channels)
    width = channels + state_maps.shape[1]
    operands = (step_raw, decay_log.reshape(1, heads), skip_gain.reshape(1, heads), gate_input,
                mixer_input, state_maps, conv_input, conv_maps)
    return call(
        functools.partial(decay_body, heads, channels // heads),
        [HBM] * len(operands),
        [((heads, tokens, tokens), F32), (square, F32), (square, F32),
         ((heads, state_maps.shape[1] // 2), F32), (square, F32), ((1, channels), F32),
         ((tokens, width), F32)],
        10**8,
        [pltpu.VMEM(x.shape, x.dtype) for x in operands]
        + [pltpu.VMEM((tokens + 8, max(channels, state_maps.shape[1])), F32),
           pltpu.SemaphoreType.DMA((len(operands),))],
    )(*operands)


def conv_body(heads, summed, leading, conv_input, conv_maps, tail, ends, values, projected, sent):
    _, channels = values.shape
    state_dim = sent.shape[1]
    count = conv_input.shape[0]
    row = lax.broadcasted_iota(jnp.int32, (8, channels), 0)
    for out, kernel, first in ((values, conv_input, 0), (projected, conv_maps, channels)):
        columns = slice(first, first + out.shape[1])
        before = leading[:, columns].astype(F32)
        early = None
        for tap in range(count - 1):
            for at in range(count - 1 - tap):
                source = LEAD - (count - 1) + tap + at
                term = kernel[tap : tap + 1, :].astype(F32) * before[source : source + 1, :]
                term = jnp.where(row == at, term, 0.0)
                early = term if early is None else early + term
        out[...] = silu(summed[:, columns]).astype(BF16)
        fixed = silu(summed[0:8, columns] + early)
        fixed = jnp.concatenate([fixed, silu(summed[8:16, columns])], axis=0)
        out[0:16, :] = fixed.astype(BF16)
    high, low = halves(values[...].astype(F32) * tail[...])
    b_maps = projected[:, :state_dim]
    state = along(high, b_maps, 0, 0) + along(low, b_maps, 0, 0)
    sent[0:channels, :] = state.astype(BF16)
    end_high, end_low = halves(ends[...])
    rest = sent.shape[0] - channels - 2 * heads
    sent[channels:, :] = jnp.concatenate(
        [end_high.astype(F32), end_low.astype(F32), jnp.zeros((rest, state_dim), F32)], axis=0
    ).astype(BF16)


def inside_body(heads, head_dim, values, projected, mix, skip, out):
    tokens, _ = values.shape
    state_dim = projected.shape[1] // 2
    scores = along(projected[:, state_dim:], projected[:, :state_dim], 1, 1)
    pair = 128 // head_dim
    for first in range(0, heads, pair):
        columns = slice(first * head_dim, (first + pair) * head_dim)
        own = values[:, columns]
        lane = lax.broadcasted_iota(jnp.int32, (tokens, pair * head_dim), 1) // head_dim
        total = None
        for k in range(pair):
            weights = (scores * mix[first + k]).astype(BF16)
            part = along(weights, own, 1, 0)
            total = part if total is None else jnp.where(lane == k, part, total)
        out[:, columns] = total + skip[:, columns] * own.astype(F32)


def fetches(blocks, at, own_weight, other_weight, held, sems):
    width = held.shape[2]
    return [
        pltpu.make_async_copy(
            source.at[:, pl.ds(pl.multiple_of(blocks[2 * at + i] * width, width), width)],
            held.at[2 * k + i],
            sems.at[2 * k + i],
        )
        for k, source in enumerate((own_weight, other_weight))
        for i in range(2)
    ]


def norm_body(
    heads, head_dim, blocks, own_weight, other_weight, projected, inside, growth, gated, gain, *rest
):
    *messages, out, part, held, sems = rest
    copies = fetches(blocks, 0, own_weight, other_weight, held, sems)
    for copy in copies:
        copy.start()
    _, width = inside.shape
    state_dim = projected.shape[1] // 2
    pieces = []
    for head in range(heads):
        rows = slice(head * head_dim, (head + 1) * head_dim)
        carried = None
        for message in messages[::-1]:
            state = message[rows, :].astype(F32)
            if carried is not None:
                ends = message[width : width + 2 * heads, :].astype(F32)
                end = ends[head : head + 1, :] + ends[heads + head : heads + head + 1, :]
                state = end * carried + state
            carried = state
        pieces.append(carried)
    high, low = halves(jnp.concatenate(pieces, axis=0))
    c_maps = projected[:, state_dim:]
    carried_part = along(c_maps, high, 1, 1) + along(c_maps, low, 1, 1)
    value = (inside[...] + carried_part * growth[...]) * gated[...]
    row = lax.broadcasted_iota(jnp.int32, (width, width), 0) // head_dim
    column = lax.broadcasted_iota(jnp.int32, (width, width), 1) // head_dim
    alike = jnp.where(row == column, 1.0, 0.0).astype(BF16)
    high, low = halves(value * value)
    mean = (along(high, alike, 1, 0) + along(low, alike, 1, 0)) / head_dim
    out[...] = (value * lax.rsqrt(mean + 1e-05) * gain[...]).astype(BF16)
    for copy in copies:
        copy.wait()
    for i in range(2):
        part[i] = along(out[...], held[i], 1, 0)


def split(total, outs):
    rows = total.shape[0] // STREAMS
    for i in range(STREAMS):
        outs[i][...] = total[i * rows : (i + 1) * rows]


def first_body(other, part, held, *outs):
    for i in range(2):
        total = part[i] + along(other[...], held[2 + i], 1, 0)
        split(total.astype(BF16), outs[i * STREAMS : (i + 1) * STREAMS])


def product_body(at, blocks, own, other, own_weight, other_weight, *rest):
    *outs, held, sems = rest
    copies = fetches(blocks, at, own_weight, other_weight, held, sems)
    for copy in copies:
        copy.start()
    for copy in copies:
        copy.wait()
    for i in range(2):
        total = along(own[...], held[i], 1, 0) + along(other[...], held[2 + i], 1, 0)
        split(total, outs[i * STREAMS : (i + 1) * STREAMS])


def project(normed, part, held, out_weight, other_weight, blocks):
    devices = lax.axis_size("tensor")
    far = devices // CORES // 2
    width = out_weight.shape[1] // devices
    tokens, depth = normed.shape
    piece = (tokens // STREAMS, width)
    other = to_other_core(normed)
    work = 8 * tokens * depth * width
    parts = call(first_body, [VMEM] * 3, [(piece, BF16)] * (2 * STREAMS), work // 2)(
        other, part, held
    )
    ups, downs = list(parts[:STREAMS]), list(parts[STREAMS:])
    for step in range(1, far + 1):
        more = step < far
        if more:
            ups[0], normed, other = lax.optimization_barrier((ups[0], normed, other))
            parts = call(
                functools.partial(product_body, step),
                [SMEM, VMEM, VMEM, HBM, HBM],
                [(piece, F32)] * (2 * STREAMS),
                work,
                [pltpu.VMEM((4, depth, width), BF16), pltpu.SemaphoreType.DMA((4,))],
            )(blocks, normed, other, out_weight, other_weight)
        for i in range(STREAMS):
            ups[i] = to_chip(ups[i], 1)
            if more:
                ups[i] = (ups[i].astype(F32) + parts[i]).astype(BF16)
                downs[i] = to_chip(downs[i], -1).astype(F32) + parts[STREAMS + i]
                if step + 1 < far:
                    downs[i] = downs[i].astype(BF16)
    return jnp.concatenate(
        [(downs[i] + ups[i].astype(F32)).astype(BF16) for i in range(STREAMS)], axis=0
    )


def local(
    mixer_input,
    state_maps,
    gate_input,
    step_raw,
    decay_log,
    skip_gain,
    conv_input,
    conv_maps,
    norm_gain,
    out_weight,
):
    tokens, channels = mixer_input.shape
    heads = decay_log.shape[0]
    head_dim = channels // heads
    state_dim = state_maps.shape[1] // 2
    square = (tokens, channels)
    devices = lax.axis_size("tensor")
    chips = devices // CORES
    far = chips // 2
    steps = jnp.arange(far)
    offsets = jnp.stack([far - steps, jnp.where(steps < far - 1, steps + 1 - far, 0)], axis=1)
    blocks = lax.rem(
        lax.axis_index("tensor") + CORES * (offsets.reshape(-1) + chips), devices
    ).astype(jnp.int32)
    ending, step_raw = lax.optimization_barrier((tail_of(mixer_input, state_maps), step_raw))
    leading = shifted(ending, "seq", 1)
    mix, tail, growth, ends, gated, skip, summed = decay(
        step_raw, decay_log, skip_gain, gate_input, mixer_input, state_maps, conv_input,
        conv_maps,
    )
    gated, out_weight, blocks = lax.optimization_barrier((gated, out_weight, blocks))
    other_weight = to_other_core(out_weight)
    rows = channels + 16 * pl.cdiv(2 * heads, 16)
    values, projected, sent = call(
        functools.partial(conv_body, heads),
        [VMEM] * 6,
        [(square, BF16), (state_maps.shape, BF16), ((rows, state_dim), BF16)],
        10**8,
    )(summed, leading, conv_input, conv_maps, tail, ends)
    messages = [shifted(sent, "seq", by) for by in range(1, lax.axis_size("seq"))]
    (inside,) = call(
        functools.partial(inside_body, heads, head_dim), [VMEM] * 4, [(square, F32)], 10**9
    )(values, projected, mix, skip)
    width = out_weight.shape[1] // devices
    normed, part, held = call(
        functools.partial(norm_body, heads, head_dim),
        [SMEM, HBM, HBM] + [VMEM] * (5 + len(messages)),
        [(square, BF16), ((2, tokens, width), F32), ((4, channels, width), BF16)],
        10**8,
        [pltpu.SemaphoreType.DMA((4,))],
    )(blocks, out_weight, other_weight, projected, inside, growth, gated,
      norm_gain.reshape(1, channels), *messages)
    return project(normed, part, held, out_weight, other_weight, blocks)


def solution(mesh):
    placed = (
        P(("group", "seq"), "tensor"),
        P(("group", "seq"), None),
        P(("group", "seq"), "tensor"),
        P("tensor", ("group", "seq")),
        P("tensor"),
        P("tensor"),
        P(None, "tensor"),
        P(),
        P("tensor"),
        P("tensor", None),
    )

    return jax.shard_map(
        local, mesh=mesh, in_specs=placed, out_specs=P(("group", "seq"), "tensor"), check_vma=False
    )
```

```python
import functools

import jax
import jax.numpy as jnp
from jax import lax
from jax.experimental import pallas as pl
from jax.experimental.pallas import tpu as pltpu
from jax.sharding import PartitionSpec as P


CORES = 2
LEAD = 16
F32 = jnp.float32
BF16 = jnp.bfloat16
PRECISE = lax.Precision.HIGHEST
VMEM = pl.BlockSpec(memory_space=pltpu.VMEM)
SMEM = pl.BlockSpec(memory_space=pltpu.SMEM)
HBM = pl.BlockSpec(memory_space=pltpu.HBM)


def shifted(shard, axis, by):
    devices = lax.axis_size(axis)
    pairs = [(i, i + by) for i in range(devices) if 0 <= i + by < devices]
    return lax.ppermute(shard, axis, pairs)


def to_other_core(shard):
    devices = lax.axis_size("tensor")
    return lax.ppermute(shard, "tensor", [(i, i ^ 1) for i in range(devices)])


def to_chip(shard, by, core):
    devices = lax.axis_size("tensor")
    first = CORES - 1
    pairs = [(i, (i - first + CORES * by + core) % devices) for i in range(first, devices, CORES)]
    return lax.ppermute(shard, "tensor", pairs)


def in_hbm(x):
    return pltpu.with_memory_space_constraint(x, pltpu.HBM)


def call(body, specs, shapes, flops, scratch=(), grant=16 << 20):
    return pl.pallas_call(
        body,
        in_specs=specs,
        out_specs=tuple(VMEM for _ in shapes),
        out_shape=tuple(jax.ShapeDtypeStruct(s, d) for s, d in shapes),
        scratch_shapes=list(scratch),
        compiler_params=pltpu.CompilerParams(vmem_limit_bytes=grant),
        cost_estimate=pl.CostEstimate(flops=flops, bytes_accessed=1 << 20, transcendentals=0),
    )


def along(a, b, ca, cb, precision=None):
    return lax.dot_general(
        a, b, (((ca,), (cb,)), ((), ())), preferred_element_type=F32, precision=precision
    )


def halves(x):
    high = x.astype(BF16)
    return high, (x - high.astype(F32)).astype(BF16)


def silu(v):
    return v / (1.0 + jnp.exp(-v))


def per_head(columns, rows, width, head_dim):
    lane = lax.broadcasted_iota(jnp.int32, (rows, width), 1) // head_dim
    spread = jnp.broadcast_to(columns[:, 0:1], (rows, width))
    for head in range(1, width // head_dim):
        spread = jnp.where(lane == head, columns[:, head : head + 1], spread)
    return spread


def tail_body(mixer, maps, out, sems):
    tokens, width = mixer.shape
    rows = pl.ds(tokens - LEAD, LEAD)
    copies = [
        pltpu.make_async_copy(mixer.at[rows], out.at[:, pl.ds(0, width)], sems.at[0]),
        pltpu.make_async_copy(maps.at[rows], out.at[:, pl.ds(width, maps.shape[1])], sems.at[1]),
    ]
    for copy in copies:
        copy.start()
    for copy in copies:
        copy.wait()


def tail_of(mixer_input, state_maps):
    width = mixer_input.shape[1] + state_maps.shape[1]
    return call(
        tail_body, [HBM, HBM], [((LEAD, width), BF16)], 1000, [pltpu.SemaphoreType.DMA((2,))],
    )(in_hbm(mixer_input), in_hbm(state_maps))[0]


def decay_body(
    heads, head_dim, step_hbm, decay_hbm, skip_hbm, gate_hbm, mixer_hbm, maps_hbm, taps_hbm,
    map_taps_hbm, mix, tail, growth, ends, gated, skip, summed, wide_taps,
    raw, logs, gains, gate, mixer, maps, taps, map_taps, padded, sems
):
    pairs = [(decay_hbm, logs), (step_hbm, raw), (skip_hbm, gains), (gate_hbm, gate),
             (taps_hbm, taps), (map_taps_hbm, map_taps), (mixer_hbm, mixer), (maps_hbm, maps)]
    copies = [pltpu.make_async_copy(a, b, sems.at[i]) for i, (a, b) in enumerate(pairs)]
    for copy in copies:
        copy.start()
    tokens = raw.shape[1]
    width = heads * head_dim
    row = lax.broadcasted_iota(jnp.int32, (heads, tokens), 0)
    to = lax.broadcasted_iota(jnp.int32, (tokens, tokens), 0)
    since = lax.broadcasted_iota(jnp.int32, (tokens, tokens), 1)
    causal = to >= since
    ones = jnp.where(causal, 1.0, 0.0).astype(F32)
    same = jnp.where(to == since, 1.0, 0.0).astype(F32)
    for copy in copies[:3]:
        copy.wait()
    step = jnp.maximum(raw[...], 0.0) + jnp.log1p(jnp.exp(-jnp.abs(raw[...])))
    rates = jnp.broadcast_to(logs[:, 0:1], (heads, tokens))
    for head in range(1, heads):
        rates = jnp.where(row == head, logs[:, head : head + 1], rates)
    change = -jnp.exp(rates) * step
    across = along(change, ones, 1, 1, PRECISE)
    down = along(ones, change, 1, 1, PRECISE)
    step_down = along(same, step, 1, 1, PRECISE)
    for head in range(heads):
        spacing = jnp.where(causal, down[:, head : head + 1] - across[head : head + 1, :], -1e30)
        mix[head] = jnp.exp(spacing) * step[head : head + 1, :]
    last = down[tokens - 1 : tokens, :]
    tail[...] = per_head(jnp.exp(last - down) * step_down, tokens, width, head_dim)
    growth[...] = per_head(jnp.exp(down), tokens, width, head_dim)
    ends[...] = jnp.broadcast_to(jnp.exp(across[:, tokens - 1 : tokens]), ends.shape)
    skip[...] = per_head(gains[...], 1, width, head_dim)
    for copy in copies[3:]:
        copy.wait()
    gated[...] = silu(gate[...].astype(F32))
    for source, kernel, first in ((mixer, taps, 0), (maps, map_taps, width)):
        count = kernel.shape[0]
        columns = source.shape[1]
        padded[0:8, :columns] = jnp.zeros((8, columns), F32)
        padded[8 : 8 + tokens, :columns] = source[...].astype(F32)
        wide_taps[:, first : first + columns] = kernel[...].astype(F32)
        total = None
        for tap in range(count):
            at = 9 - count + tap
            scale = wide_taps[tap : tap + 1, first : first + columns]
            term = scale * padded[at : at + tokens, :columns]
            total = term if total is None else total + term
        summed[:, first : first + columns] = total


def decay(step_raw, decay_log, skip_gain, gate_input, mixer_input, state_maps, conv_input,
          conv_maps):
    heads, tokens = step_raw.shape
    channels = mixer_input.shape[1]
    square = (tokens, channels)
    width = channels + state_maps.shape[1]
    operands = (step_raw, decay_log.reshape(1, heads), skip_gain.reshape(1, heads), gate_input,
                mixer_input, state_maps, conv_input, conv_maps)
    return call(
        functools.partial(decay_body, heads, channels // heads),
        [HBM] * len(operands),
        [((heads, tokens, tokens), F32), (square, F32), (square, F32),
         ((heads, state_maps.shape[1] // 2), F32), (square, F32), ((1, channels), F32),
         ((tokens, width), F32), ((conv_input.shape[0], width), F32)],
        10**8,
        [pltpu.VMEM(x.shape, x.dtype) for x in operands]
        + [pltpu.VMEM((tokens + 8, max(channels, state_maps.shape[1])), F32),
           pltpu.SemaphoreType.DMA((len(operands),))],
    )(*(in_hbm(x) for x in operands))


def conv_body(heads, summed, leading, taps, tail, ends, values, projected, sent):
    _, channels = values.shape
    state_dim = sent.shape[1]
    count = taps.shape[0]
    row = lax.broadcasted_iota(jnp.int32, (8, channels), 0)
    for out, first in ((values, 0), (projected, channels)):
        columns = slice(first, first + out.shape[1])
        before = leading[:, columns].astype(F32)
        early = None
        for tap in range(count - 1):
            for at in range(count - 1 - tap):
                source = LEAD - (count - 1) + tap + at
                term = taps[tap : tap + 1, columns] * before[source : source + 1, :]
                term = jnp.where(row == at, term, 0.0)
                early = term if early is None else early + term
        out[...] = silu(summed[:, columns]).astype(BF16)
        fixed = silu(summed[0:8, columns] + early)
        fixed = jnp.concatenate([fixed, silu(summed[8:16, columns])], axis=0)
        out[0:16, :] = fixed.astype(BF16)
    high, low = halves(values[...].astype(F32) * tail[...])
    b_maps = projected[:, :state_dim]
    state = along(high, b_maps, 0, 0) + along(low, b_maps, 0, 0)
    sent[0:channels, :] = state.astype(BF16)
    end_high, end_low = halves(ends[...])
    rest = sent.shape[0] - channels - 2 * heads
    sent[channels:, :] = jnp.concatenate(
        [end_high.astype(F32), end_low.astype(F32), jnp.zeros((rest, state_dim), F32)], axis=0
    ).astype(BF16)


def inside_body(heads, head_dim, values, projected, mix, skip, out):
    tokens, _ = values.shape
    state_dim = projected.shape[1] // 2
    scores = along(projected[:, state_dim:], projected[:, :state_dim], 1, 1)
    pair = 128 // head_dim
    for first in range(0, heads, pair):
        columns = slice(first * head_dim, (first + pair) * head_dim)
        own = values[:, columns]
        lane = lax.broadcasted_iota(jnp.int32, (tokens, pair * head_dim), 1) // head_dim
        total = None
        for k in range(pair):
            weights = (scores * mix[first + k]).astype(BF16)
            part = along(weights, own, 1, 0)
            total = part if total is None else jnp.where(lane == k, part, total)
        out[:, columns] = total + skip[:, columns] * own.astype(F32)


def fetches(me, chips, bys, weights, held, sems):
    width = held.shape[2]
    copies = []
    for i, by in enumerate(bys):
        chip = lax.rem(lax.div(me[0], CORES) + by + chips, chips)
        at = pl.ds(pl.multiple_of(chip * width, width), width)
        for k, weight in enumerate(weights):
            place = len(weights) * i + k
            copies.append(
                pltpu.make_async_copy(weight.at[:, at], held.at[place], sems.at[place])
            )
    return copies


def norm_body(
    heads, head_dim, chips, bys, me, position, own_weight, other_weight, projected, inside, growth,
    gated, gain, *rest
):
    *messages, out, held, sems = rest
    copies = fetches(me, chips, bys, (own_weight, other_weight), held, sems)
    for copy in copies:
        copy.start()
    _, width = inside.shape
    state_dim = projected.shape[1] // 2
    pieces = []
    for head in range(heads):
        rows = slice(head * head_dim, (head + 1) * head_dim)
        carried = None
        for by in range(len(messages), 0, -1):
            message = messages[by - 1]
            state = message[rows, :].astype(F32)
            if carried is not None:
                ends = message[width : width + 2 * heads, :].astype(F32)
                end = ends[head : head + 1, :] + ends[heads + head : heads + head + 1, :]
                state = end * carried + state
            carried = jnp.where(position[0] >= by, state, 0.0)
        pieces.append(carried)
    high, low = halves(jnp.concatenate(pieces, axis=0))
    c_maps = projected[:, state_dim:]
    carried_part = along(c_maps, high, 1, 1) + along(c_maps, low, 1, 1)
    value = (inside[...] + carried_part * growth[...]) * gated[...]
    row = lax.broadcasted_iota(jnp.int32, (width, width), 0) // head_dim
    column = lax.broadcasted_iota(jnp.int32, (width, width), 1) // head_dim
    alike = jnp.where(row == column, 1.0, 0.0).astype(BF16)
    high, low = halves(value * value)
    mean = (along(high, alike, 1, 0) + along(low, alike, 1, 0)) / head_dim
    out[...] = (value * lax.rsqrt(mean + 1e-05) * gain[...]).astype(BF16)
    for copy in copies:
        copy.wait()


def own_body(own, held, *parts):
    for i, part in enumerate(parts):
        part[...] = along(own[...], held[2 * i], 1, 0)


def first_body(other, held, *rest):
    count = len(rest) // (1 + CORES)
    for i, part in enumerate(rest[:count]):
        total = part[...] + along(other[...], held[2 * i + 1], 1, 0)
        outs = rest[count + CORES * i : count + CORES * (i + 1)]
        width = total.shape[1] // CORES
        for core, out in enumerate(outs):
            out[...] = total[:, core * width : (core + 1) * width].astype(BF16)


def rest_body(chips, bys, me, own, other, own_weight, other_weight, *rest):
    *outs, held, mine, sems, mine_sems = rest
    weights = (own_weight, other_weight)
    width = outs[-1].shape[1]
    copies = fetches(me, chips, bys, weights, held, sems)
    at = pl.ds(pl.multiple_of(me[0] * width, width), width)
    for k, weight in enumerate(weights):
        copies.append(pltpu.make_async_copy(weight.at[:, at], mine.at[k], mine_sems.at[k]))
    for copy in copies:
        copy.start()
    for i in range(len(bys)):
        for copy in copies[2 * i : 2 * i + 2]:
            copy.wait()
        total = along(own[...], held[2 * i], 1, 0) + along(other[...], held[2 * i + 1], 1, 0)
        for core in range(CORES):
            outs[CORES * i + core][...] = total[:, core * width : (core + 1) * width]
    for copy in copies[-2:]:
        copy.wait()
    outs[-1][...] = along(own[...], mine[0], 1, 0) + along(other[...], mine[1], 1, 0)


def project(normed, held, out_weight, other_weight, me, bys):
    devices = lax.axis_size("tensor")
    chips = devices // CORES
    far = chips // 2
    width = out_weight.shape[1] // devices
    tokens, depth = normed.shape
    piece = (tokens, width)
    work = 2 * tokens * depth * width * CORES
    own = call(
        own_body, [VMEM] * 2, [((tokens, CORES * width), F32)] * len(bys), work * len(bys)
    )(normed, held)
    other = to_other_core(normed)
    parts = call(
        first_body, [VMEM] * (2 + len(bys)), [(piece, BF16)] * (CORES * len(bys)), work * len(bys)
    )(other, held, *own)
    ups, downs = list(parts[:CORES]), list(parts[CORES:])
    left = []
    for step in range(1, far):
        left += [far - step] + ([step + 1 - far] if step + 1 < far else [])
    ups[0], normed, other = lax.optimization_barrier((ups[0], normed, other))
    parts = call(
        functools.partial(rest_body, chips, left),
        [SMEM, VMEM, VMEM, HBM, HBM],
        [(piece, F32)] * (CORES * len(left) + 1),
        2 * work * len(left),
        [pltpu.VMEM((2 * len(left), depth, CORES * width), BF16),
         pltpu.VMEM((2, depth, width), BF16),
         pltpu.SemaphoreType.DMA((2 * len(left),)), pltpu.SemaphoreType.DMA((2,))],
    )(me, normed, other, in_hbm(out_weight), in_hbm(other_weight))
    part = {(by, core): parts[CORES * i + core] for i, by in enumerate(left) for core in range(CORES)}
    for step in range(1, far + 1):
        for core in range(CORES):
            ups[core] = to_chip(ups[core], 1, core if step == far else CORES - 1)
            if step < far:
                ups[core] = (ups[core].astype(F32) + part[far - step, core]).astype(BF16)
                by = step + 1 - far
                downs[core] = to_chip(downs[core], -1, CORES - 1 if by else core)
                if by:
                    downs[core] = (downs[core].astype(F32) + part[by, core]).astype(BF16)
    total = parts[-1]
    for arrived in downs + ups:
        total = total + arrived.astype(F32)
    return total.astype(BF16)


def local(
    mixer_input,
    state_maps,
    gate_input,
    step_raw,
    decay_log,
    skip_gain,
    conv_input,
    conv_maps,
    norm_gain,
    out_weight,
):
    tokens, channels = mixer_input.shape
    heads = decay_log.shape[0]
    head_dim = channels // heads
    state_dim = state_maps.shape[1] // 2
    square = (tokens, channels)
    me = lax.axis_index("tensor").reshape(1)
    position = lax.axis_index("seq").reshape(1)
    ending, step_raw = lax.optimization_barrier((tail_of(mixer_input, state_maps), step_raw))
    leading = shifted(ending, "seq", 1)
    mix, tail, growth, ends, gated, skip, summed, taps = decay(
        step_raw, decay_log, skip_gain, gate_input, mixer_input, state_maps, conv_input,
        conv_maps,
    )
    gated, out_weight = lax.optimization_barrier((gated, out_weight))
    other_weight = to_other_core(out_weight)
    rows = channels + 16 * pl.cdiv(2 * heads, 16)
    values, projected, sent = call(
        functools.partial(conv_body, heads),
        [VMEM] * 5,
        [(square, BF16), (state_maps.shape, BF16), ((rows, state_dim), BF16)],
        10**8,
    )(summed, leading, taps, tail, ends)
    pieces = lax.axis_size("seq")
    messages = [
        lax.ppermute(sent, "seq", [(i, (i + by) % pieces) for i in range(pieces)])
        for by in range(1, pieces)
    ]
    (inside,) = call(
        functools.partial(inside_body, heads, head_dim), [VMEM] * 4, [(square, F32)], 10**9
    )(values, projected, mix, skip)
    devices = lax.axis_size("tensor")
    chips = devices // CORES
    width = out_weight.shape[1] // chips
    bys = (chips // 2, 1 - chips // 2)
    count = CORES * len(bys)
    normed, held = call(
        functools.partial(norm_body, heads, head_dim, chips, bys),
        [SMEM, SMEM, HBM, HBM] + [VMEM] * (5 + len(messages)),
        [(square, BF16), ((count, channels, width), BF16)],
        10**8,
        [pltpu.SemaphoreType.DMA((count,))],
    )(me, position, in_hbm(out_weight), in_hbm(other_weight), projected, inside, growth, gated,
      norm_gain.reshape(1, channels), *messages)
    return project(normed, held, out_weight, other_weight, me, bys)


def solution(mesh):
    placed = (
        P(("group", "seq"), "tensor"),
        P(("group", "seq"), None),
        P(("group", "seq"), "tensor"),
        P("tensor", ("group", "seq")),
        P("tensor"),
        P("tensor"),
        P(None, "tensor"),
        P(),
        P("tensor"),
        P("tensor", None),
    )

    return jax.shard_map(
        local, mesh=mesh, in_specs=placed, out_specs=P(("group", "seq"), "tensor"), check_vma=False
    )
```

```python
import functools

import jax
import jax.numpy as jnp
from jax import lax
from jax.experimental import pallas as pl
from jax.experimental.pallas import tpu as pltpu
from jax.sharding import PartitionSpec as P


CORES = 2
LEAD = 16
STREAMS = 2
F32 = jnp.float32
BF16 = jnp.bfloat16
PRECISE = lax.Precision.HIGHEST
VMEM = pl.BlockSpec(memory_space=pltpu.VMEM)
SMEM = pl.BlockSpec(memory_space=pltpu.SMEM)
HBM = pl.BlockSpec(memory_space=pltpu.HBM)


def shifted(shard, axis, by):
    devices = lax.axis_size(axis)
    pairs = [(i, i + by) for i in range(devices) if 0 <= i + by < devices]
    return lax.ppermute(shard, axis, pairs)


def to_other_core(shard):
    devices = lax.axis_size("tensor")
    return lax.ppermute(shard, "tensor", [(i, i ^ 1) for i in range(devices)])


def to_chip(shard, by):
    devices = lax.axis_size("tensor")
    return lax.ppermute(
        shard, "tensor", [(i, (i + CORES * by) % devices) for i in range(devices)]
    )


def in_hbm(x):
    return pltpu.with_memory_space_constraint(x, pltpu.HBM)


def call(body, specs, shapes, flops, scratch=(), grant=16 << 20):
    return pl.pallas_call(
        body,
        in_specs=specs,
        out_specs=tuple(VMEM for _ in shapes),
        out_shape=tuple(jax.ShapeDtypeStruct(s, d) for s, d in shapes),
        scratch_shapes=list(scratch),
        compiler_params=pltpu.CompilerParams(vmem_limit_bytes=grant),
        cost_estimate=pl.CostEstimate(flops=flops, bytes_accessed=1 << 20, transcendentals=0),
    )


def along(a, b, ca, cb, precision=None):
    return lax.dot_general(
        a, b, (((ca,), (cb,)), ((), ())), preferred_element_type=F32, precision=precision
    )


def halves(x):
    high = x.astype(BF16)
    return high, (x - high.astype(F32)).astype(BF16)


def silu(v):
    return v / (1.0 + jnp.exp(-v))


def per_head(columns, rows, width, head_dim):
    lane = lax.broadcasted_iota(jnp.int32, (rows, width), 1) // head_dim
    spread = jnp.broadcast_to(columns[:, 0:1], (rows, width))
    for head in range(1, width // head_dim):
        spread = jnp.where(lane == head, columns[:, head : head + 1], spread)
    return spread


def tail_body(mixer, maps, out, sems):
    tokens, width = mixer.shape
    rows = pl.ds(tokens - LEAD, LEAD)
    copies = [
        pltpu.make_async_copy(mixer.at[rows], out.at[:, pl.ds(0, width)], sems.at[0]),
        pltpu.make_async_copy(maps.at[rows], out.at[:, pl.ds(width, maps.shape[1])], sems.at[1]),
    ]
    for copy in copies:
        copy.start()
    for copy in copies:
        copy.wait()


def tail_of(mixer_input, state_maps):
    width = mixer_input.shape[1] + state_maps.shape[1]
    return call(
        tail_body, [HBM, HBM], [((LEAD, width), BF16)], 1000, [pltpu.SemaphoreType.DMA((2,))],
    )(in_hbm(mixer_input), in_hbm(state_maps))[0]


def spread_over(vectors, tokens):
    heads = vectors.shape[1]
    row = lax.broadcasted_iota(jnp.int32, (heads, tokens), 0)
    spread = jnp.broadcast_to(vectors[:, 0:1], (heads, tokens))
    for head in range(1, heads):
        spread = jnp.where(row == head, vectors[:, head : head + 1], spread)
    return spread


def decay_body(
    head_dim, step_hbm, decay_hbm, taps_hbm, map_taps_hbm, mixer_hbm, maps_hbm,
    tail, ends, summed, wide_taps, across, down, step,
    raw, logs, taps, map_taps, mixer, maps, padded, sems
):
    pairs = [(decay_hbm, logs), (step_hbm, raw), (taps_hbm, taps), (map_taps_hbm, map_taps),
             (mixer_hbm, mixer), (maps_hbm, maps)]
    copies = [pltpu.make_async_copy(a, b, sems.at[i]) for i, (a, b) in enumerate(pairs)]
    for copy in copies:
        copy.start()
    heads, tokens = raw.shape
    width = heads * head_dim
    to = lax.broadcasted_iota(jnp.int32, (tokens, tokens), 0)
    since = lax.broadcasted_iota(jnp.int32, (tokens, tokens), 1)
    ones = jnp.where(to >= since, 1.0, 0.0).astype(F32)
    same = jnp.where(to == since, 1.0, 0.0).astype(F32)
    for copy in copies[:2]:
        copy.wait()
    step[...] = jnp.maximum(raw[...], 0.0) + jnp.log1p(jnp.exp(-jnp.abs(raw[...])))
    change = -jnp.exp(spread_over(logs[...], tokens)) * step[...]
    across[...] = along(change, ones, 1, 1, PRECISE)
    down[...] = along(ones, change, 1, 1, PRECISE)
    step_down = along(same, step[...], 1, 1, PRECISE)
    last = down[tokens - 1 : tokens, :]
    tail[...] = per_head(jnp.exp(last - down[...]) * step_down, tokens, width, head_dim)
    ends[...] = jnp.broadcast_to(jnp.exp(across[:, tokens - 1 : tokens]), ends.shape)
    for copy in copies[2:]:
        copy.wait()
    for source, kernel, first in ((mixer, taps, 0), (maps, map_taps, width)):
        count = kernel.shape[0]
        columns = source.shape[1]
        padded[0:8, :columns] = jnp.zeros((8, columns), F32)
        padded[8 : 8 + tokens, :columns] = source[...].astype(F32)
        wide_taps[:, first : first + columns] = kernel[...].astype(F32)
        total = None
        for tap in range(count):
            at = 9 - count + tap
            scale = wide_taps[tap : tap + 1, first : first + columns]
            term = scale * padded[at : at + tokens, :columns]
            total = term if total is None else total + term
        summed[:, first : first + columns] = total


def decay(step_raw, decay_log, mixer_input, state_maps, conv_input, conv_maps):
    heads, tokens = step_raw.shape
    channels = mixer_input.shape[1]
    width = channels + state_maps.shape[1]
    operands = (step_raw, decay_log.reshape(1, heads), conv_input, conv_maps, mixer_input,
                state_maps)
    scratch = (step_raw, operands[1], conv_input, conv_maps, mixer_input, state_maps)
    return call(
        functools.partial(decay_body, channels // heads),
        [HBM] * len(operands),
        [((tokens, channels), F32), ((heads, state_maps.shape[1] // 2), F32),
         ((tokens, width), F32), ((conv_input.shape[0], width), F32),
         ((heads, tokens), F32), ((tokens, heads), F32), ((heads, tokens), F32)],
        10**8,
        [pltpu.VMEM(x.shape, x.dtype) for x in scratch]
        + [pltpu.VMEM((tokens + 8, max(channels, state_maps.shape[1])), F32),
           pltpu.SemaphoreType.DMA((len(operands),))],
    )(*(in_hbm(x) for x in operands))


def conv_body(heads, summed, leading, taps, tail, ends, values, projected, sent):
    _, channels = values.shape
    state_dim = sent.shape[1]
    count = taps.shape[0]
    row = lax.broadcasted_iota(jnp.int32, (8, channels), 0)
    for out, first in ((values, 0), (projected, channels)):
        columns = slice(first, first + out.shape[1])
        before = leading[:, columns].astype(F32)
        early = None
        for tap in range(count - 1):
            for at in range(count - 1 - tap):
                source = LEAD - (count - 1) + tap + at
                term = taps[tap : tap + 1, columns] * before[source : source + 1, :]
                term = jnp.where(row == at, term, 0.0)
                early = term if early is None else early + term
        out[...] = silu(summed[:, columns]).astype(BF16)
        fixed = silu(summed[0:8, columns] + early)
        fixed = jnp.concatenate([fixed, silu(summed[8:16, columns])], axis=0)
        out[0:16, :] = fixed.astype(BF16)
    high, low = halves(values[...].astype(F32) * tail[...])
    b_maps = projected[:, :state_dim]
    state = along(high, b_maps, 0, 0) + along(low, b_maps, 0, 0)
    sent[0:channels, :] = state.astype(BF16)
    end_high, end_low = halves(ends[...])
    rest = sent.shape[0] - channels - 2 * heads
    sent[channels:, :] = jnp.concatenate(
        [end_high.astype(F32), end_low.astype(F32), jnp.zeros((rest, state_dim), F32)], axis=0
    ).astype(BF16)


def inside_body(
    heads, head_dim, values, projected, across, down, step, gate_hbm, skip_hbm, out, growth, gated,
    gate, gains, sems
):
    copies = [pltpu.make_async_copy(gate_hbm, gate, sems.at[0]),
              pltpu.make_async_copy(skip_hbm, gains, sems.at[1])]
    for copy in copies:
        copy.start()
    tokens, width = values.shape
    state_dim = projected.shape[1] // 2
    scores = along(projected[:, state_dim:], projected[:, :state_dim], 1, 1)
    to = lax.broadcasted_iota(jnp.int32, (tokens, tokens), 0)
    since = lax.broadcasted_iota(jnp.int32, (tokens, tokens), 1)
    causal = to >= since
    growth[...] = per_head(jnp.exp(down[...]), tokens, width, head_dim)
    for copy in copies:
        copy.wait()
    gated[...] = silu(gate[...].astype(F32))
    skip = per_head(gains[...], 1, width, head_dim)
    pair = 128 // head_dim
    for first in range(0, heads, pair):
        columns = slice(first * head_dim, (first + pair) * head_dim)
        own = values[:, columns]
        lane = lax.broadcasted_iota(jnp.int32, (tokens, pair * head_dim), 1) // head_dim
        total = None
        for k in range(pair):
            head = slice(first + k, first + k + 1)
            spacing = jnp.where(causal, down[:, head] - across[head, :], -1e30)
            weights = (scores * (jnp.exp(spacing) * step[head, :])).astype(BF16)
            part = along(weights, own, 1, 0)
            total = part if total is None else jnp.where(lane == k, part, total)
        out[:, columns] = total + skip[:, columns] * own.astype(F32)


def fetches(me, devices, bys, weights, held, sems):
    width = held.shape[2]
    copies = []
    for i, by in enumerate(bys):
        block = lax.rem(me[0] + CORES * by + devices, devices)
        at = pl.ds(pl.multiple_of(block * width, width), width)
        for k, weight in enumerate(weights):
            place = len(weights) * i + k
            copies.append(
                pltpu.make_async_copy(weight.at[:, at], held.at[place], sems.at[place])
            )
    return copies


def norm_body(
    heads, head_dim, devices, bys, me, position, own_weight, other_weight, projected, inside, growth,
    gated, gain, *rest
):
    *messages, out, held, sems = rest
    copies = fetches(me, devices, bys, (own_weight, other_weight), held, sems)
    for copy in copies:
        copy.start()
    _, width = inside.shape
    state_dim = projected.shape[1] // 2
    pieces = []
    for head in range(heads):
        rows = slice(head * head_dim, (head + 1) * head_dim)
        carried = None
        for by in range(len(messages), 0, -1):
            message = messages[by - 1]
            state = message[rows, :].astype(F32)
            if carried is not None:
                ends = message[width : width + 2 * heads, :].astype(F32)
                end = ends[head : head + 1, :] + ends[heads + head : heads + head + 1, :]
                state = end * carried + state
            carried = jnp.where(position[0] >= by, state, 0.0)
        pieces.append(carried)
    high, low = halves(jnp.concatenate(pieces, axis=0))
    c_maps = projected[:, state_dim:]
    carried_part = along(c_maps, high, 1, 1) + along(c_maps, low, 1, 1)
    value = (inside[...] + carried_part * growth[...]) * gated[...]
    row = lax.broadcasted_iota(jnp.int32, (width, width), 0) // head_dim
    column = lax.broadcasted_iota(jnp.int32, (width, width), 1) // head_dim
    alike = jnp.where(row == column, 1.0, 0.0).astype(BF16)
    high, low = halves(value * value)
    mean = (along(high, alike, 1, 0) + along(low, alike, 1, 0)) / head_dim
    out[...] = (value * lax.rsqrt(mean + 1e-05) * gain[...]).astype(BF16)
    for copy in copies:
        copy.wait()


def own_body(own, held, *parts):
    for i, part in enumerate(parts):
        part[...] = along(own[...], held[2 * i], 1, 0)


def split(total, outs):
    rows = total.shape[0] // len(outs)
    for i, out in enumerate(outs):
        out[...] = total[i * rows : (i + 1) * rows].astype(out.dtype)


def first_body(other, held, *rest):
    count = len(rest) // (1 + STREAMS)
    for i, part in enumerate(rest[:count]):
        total = part[...] + along(other[...], held[2 * i + 1], 1, 0)
        split(total, rest[count + STREAMS * i : count + STREAMS * (i + 1)])


def rest_body(devices, bys, me, own, other, own_weight, other_weight, *outs):
    width = outs[0].shape[1]
    for i, by in enumerate(bys):
        block = lax.rem(me[0] + CORES * by + devices, devices)
        at = pl.ds(pl.multiple_of(block * width, width), width)
        total = along(own[...], own_weight[:, at], 1, 0)
        total = total + along(other[...], other_weight[:, at], 1, 0)
        split(total, outs[STREAMS * i : STREAMS * (i + 1)])


def project(normed, held, out_weight, other_weight, me, bys):
    devices = lax.axis_size("tensor")
    far = devices // CORES // 2
    width = out_weight.shape[1] // devices
    tokens, depth = normed.shape
    piece = (tokens // STREAMS, width)
    work = 2 * tokens * depth * width
    own = call(own_body, [VMEM] * 2, [((tokens, width), F32)] * len(bys), work * len(bys))(
        normed, held
    )
    other = to_other_core(normed)
    parts = call(
        first_body, [VMEM] * (2 + len(bys)), [(piece, BF16)] * (STREAMS * len(bys)),
        work * len(bys),
    )(other, held, *own)
    ups, downs = list(parts[:STREAMS]), list(parts[STREAMS:])
    left = []
    for step in range(1, far):
        left += [far - step, step + 1 - far]
    ups[0], normed, other = lax.optimization_barrier((ups[0], normed, other))
    parts = call(
        functools.partial(rest_body, devices, left),
        [SMEM] + [VMEM] * 4,
        [(piece, F32)] * (STREAMS * len(left)),
        2 * work * len(left),
    )(me, normed, other, out_weight, other_weight)
    part = {
        (by, i): parts[STREAMS * k + i] for k, by in enumerate(left) for i in range(STREAMS)
    }
    for step in range(1, far + 1):
        for i in range(STREAMS):
            ups[i] = to_chip(ups[i], 1)
            if step < far:
                ups[i] = (ups[i].astype(F32) + part[far - step, i]).astype(BF16)
                downs[i] = to_chip(downs[i], -1).astype(F32) + part[step + 1 - far, i]
                if step + 1 < far:
                    downs[i] = downs[i].astype(BF16)
    return jnp.concatenate(
        [(downs[i] + ups[i].astype(F32)).astype(BF16) for i in range(STREAMS)], axis=0
    )


def local(
    mixer_input,
    state_maps,
    gate_input,
    step_raw,
    decay_log,
    skip_gain,
    conv_input,
    conv_maps,
    norm_gain,
    out_weight,
):
    tokens, channels = mixer_input.shape
    heads = decay_log.shape[0]
    head_dim = channels // heads
    state_dim = state_maps.shape[1] // 2
    square = (tokens, channels)
    me = lax.axis_index("tensor").reshape(1)
    position = lax.axis_index("seq").reshape(1)
    ending, step_raw = lax.optimization_barrier((tail_of(mixer_input, state_maps), step_raw))
    leading = shifted(ending, "seq", 1)
    tail, ends, summed, taps, across, down, step = decay(
        step_raw, decay_log, mixer_input, state_maps, conv_input, conv_maps
    )
    step, out_weight = lax.optimization_barrier((step, out_weight))
    other_weight = to_other_core(out_weight)
    rows = channels + 16 * pl.cdiv(2 * heads, 16)
    values, projected, sent = call(
        functools.partial(conv_body, heads),
        [VMEM] * 5,
        [(square, BF16), (state_maps.shape, BF16), ((rows, state_dim), BF16)],
        10**8,
    )(summed, leading, taps, tail, ends)
    pieces = lax.axis_size("seq")
    messages = [
        lax.ppermute(sent, "seq", [(i, (i + by) % pieces) for i in range(pieces)])
        for by in range(1, pieces)
    ]
    inside, growth, gated = call(
        functools.partial(inside_body, heads, head_dim),
        [VMEM] * 5 + [HBM] * 2,
        [(square, F32)] * 3,
        10**9,
        [pltpu.VMEM(square, BF16), pltpu.VMEM((1, heads), F32), pltpu.SemaphoreType.DMA((2,))],
    )(values, projected, across, down, step, in_hbm(gate_input), in_hbm(skip_gain.reshape(1, heads)))
    devices = lax.axis_size("tensor")
    width = out_weight.shape[1] // devices
    far = devices // CORES // 2
    bys = (far, 1 - far)
    count = 2 * len(bys)
    normed, held = call(
        functools.partial(norm_body, heads, head_dim, devices, bys),
        [SMEM, SMEM, HBM, HBM] + [VMEM] * (5 + len(messages)),
        [(square, BF16), ((count, channels, width), BF16)],
        10**8,
        [pltpu.SemaphoreType.DMA((count,))],
    )(me, position, in_hbm(out_weight), in_hbm(other_weight), projected, inside, growth, gated,
      norm_gain.reshape(1, channels), *messages)
    return project(normed, held, out_weight, other_weight, me, bys)


def solution(mesh):
    placed = (
        P(("group", "seq"), "tensor"),
        P(("group", "seq"), None),
        P(("group", "seq"), "tensor"),
        P("tensor", ("group", "seq")),
        P("tensor"),
        P("tensor"),
        P(None, "tensor"),
        P(),
        P("tensor"),
        P("tensor", None),
    )

    return jax.shard_map(
        local, mesh=mesh, in_specs=placed, out_specs=P(("group", "seq"), "tensor"), check_vma=False
    )
```
